32 devices in a mesh: rep: 8 (over z, x), rows: 4 (over y, core).
Axes of the slice: x: 2, y: 2, z: 4, core: 2. Of those that a mesh axis runs over, the one named last changes fastest.
Arguments:
- item_table: bfloat16 [131072, 128], P(('rep', 'rows')), may hold values from -6 to 6
- history_ids: int32 [512, 64], P('rows'), may hold values from 0 to 131071, as said below
- history_mask: int32 [512, 64], P('rows'), may hold values 0 or 1
Outputs:
- user_vectors: float32 [512, 128], P('rows')
The draws below stay inside these ranges and needn't reach their ends.
Inputs may be any that keep to these rules, and one draw needn't show every extreme that they name: `history_ids`: among the slots of the 128 bags of one index of rows (bags b * 128 to (b + 1) * 128 - 1), exactly 256 ids fall in each block of 4096 consecutive table rows, used or not.
All inputs are finite; a program needn't handle non-finite values. No bound on the sum of `history_mask` on one device may be relied on, other than what follows from the above.
Results may differ from the reference program's by a relative error of at most 0.0017.
Values may be sent and summed in bfloat16 or wider, within the bound.
No kernel may reach another device: no remote copies, remote signals or barrier semaphores. Data moves between devices by JAX's collectives and lax.ppermute only.
A program may use at most 128 MiB of HBM per device.

```python
import jax
import jax.numpy as jnp
from jax import lax

D = 128
L = 64
ROWS_DEV = 4096
B_DEV = 128
BAGS = 512
VOCAB = 131072
DEVICES = 32


def draw_history_ids(key, part):
    nblock = BAGS // B_DEV
    slots = B_DEV * L
    keys = jax.random.split(jax.random.fold_in(key, 7), nblock)
    base = jnp.arange(slots, dtype=jnp.int32) % DEVICES
    owners = jax.vmap(lambda single: jax.random.permutation(single, base))(keys)
    offsets = jax.random.randint(jax.random.fold_in(key, 11), (nblock, slots), 0, ROWS_DEV, dtype=jnp.int32)
    return (owners * ROWS_DEV + offsets).reshape(BAGS, L)


def with_ends(drawn, key, smallest, largest):
    dims = drawn.shape
    spot = [jax.random.randint(jax.random.fold_in(key, axis), (), 0, dims[axis]) for axis in range(len(dims))]
    drawn = drawn.at[tuple(spot)].set(smallest)
    longest = dims.index(max(dims))
    spot[longest] = (spot[longest] + 1) % dims[longest]
    return drawn.at[tuple(spot)].set(largest)


def shard_levels(stream_key, extent, shards, least, largest):
    loudness = 1.0
    for axis_at, blocks in shards:
        heights = jax.random.uniform(jax.random.fold_in(jax.random.fold_in(stream_key, 6), axis_at), (blocks,), jnp.float32, least / len(shards), largest / len(shards))
        loudness = loudness * jnp.repeat(jnp.exp(heights), extent[axis_at] // blocks).reshape((-1,) + (1,) * (len(extent) - 1 - axis_at))
    return loudness


def gaussian(rng, shape, spread, reach, cuts=(), kind=jnp.bfloat16):
    array = spread * jax.random.normal(rng, shape, jnp.float32)
    if cuts:
        array = array * shard_levels(rng, shape, cuts, -0.22, 0.18)
    return jnp.clip(array, -reach, reach).astype(kind)


def setup_inputs(seed: int = 0) -> dict:
    arg_keys = jax.random.split(jax.random.key(seed), 4)
    return {
        "item_table": gaussian(arg_keys[0], (VOCAB, D), 1.0, 6.0, ((0, 32),)),
        "history_ids": draw_history_ids(jax.random.fold_in(arg_keys[3], 71), 0),
        "history_mask": with_ends((jax.random.randint(arg_keys[2], (BAGS, L), 0, 4) < 3).astype(jnp.int32), jax.random.fold_in(arg_keys[2], 1), 0, 1),
    }


def reference(item_table, history_ids, history_mask):
    rows = item_table[history_ids].astype(jnp.float32)
    weights = history_mask.astype(jnp.float32)[:, :, None]
    pooled = lax.optimization_barrier(jnp.sum(rows * weights, axis=1))
    scale = 1.0 / jnp.sqrt(lax.optimization_barrier(jnp.mean(pooled * pooled, axis=1, keepdims=True)) + 1e-06)
    return pooled * scale
```

```python
import functools

import jax
import jax.numpy as jnp
from jax import lax
from jax.experimental import pallas as pl
from jax.experimental.pallas import tpu as pltpu
from jax.sharding import PartitionSpec as P

LANES = 128
LOW = 256


def pool_kernel(base_ref, *refs, groups, highs, length, unroll):
    key_refs = refs[:groups]
    table_ref, out_ref, m_ref, low_ref, cnt0_ref, cnt1_ref = refs[groups:]
    per = LANES // length
    nbags = key_refs[0].shape[1]
    prow = nbags // per
    base = base_ref[0]
    lane = lax.broadcasted_iota(jnp.int32, (prow, LANES), 1)
    odd = lax.broadcasted_iota(jnp.int32, (prow, LANES), 0) & 1
    for g in range(groups):
        keys = jnp.concatenate([key_refs[g][...]] * per, axis=0).T
        packed = keys[:prow]
        for j in range(1, per):
            packed = jnp.where(lane >= j * length, keys[j * prow : (j + 1) * prow], packed)
        local = packed - base
        inside = (local >= 0) & (local < highs * LOW)
        m = lax.shift_right_arithmetic(local, LOW.bit_length() - 1) + highs * (lane // length + per * odd)
        m_ref[g * prow : (g + 1) * prow, :] = jnp.where(inside, m, -1).astype(jnp.float32)
        low_ref[g * prow : (g + 1) * prow, :] = jnp.where(inside, local & (LOW - 1), -1).astype(jnp.float32)

    def numbered(n):
        return lax.broadcasted_iota(jnp.int32, (n, LANES), 0).astype(jnp.float32).astype(jnp.bfloat16)

    iota_m, iota_low = numbered(2 * per * highs), numbered(LOW)
    one, zero = jnp.bfloat16(1), jnp.bfloat16(0)

    def hot(row, iota):
        row = jnp.broadcast_to(row, (16, LANES)).astype(jnp.bfloat16)
        tiles = [jnp.where(iota[k : k + 16] == row, one, zero) for k in range(0, iota.shape[0], 16)]
        return jnp.concatenate(tiles, axis=0)

    def step(c, carry):
        for u in range(unroll):
            p = (c * unroll + u) * 2
            pair = [pl.ds(p, 1), pl.ds(p + 1, 1)]
            lhs = jnp.concatenate([hot(m_ref[at, :], iota_m) for at in pair], axis=1)
            rhs = jnp.concatenate([hot(low_ref[at, :], iota_low) for at in pair], axis=1)
            cnt = lax.dot_general(lhs, rhs, (((1,), (1,)), ((), ())), preferred_element_type=jnp.float32)
            g = p // prow
            for i in range(2 * per):
                bag = g * nbags + (i % per) * prow + (p - g * prow) + i // per
                at = pl.ds(pl.multiple_of(bag * highs, highs), highs)
                cnt0_ref[at, :] = cnt[i * highs : (i + 1) * highs, :LANES]
                cnt1_ref[at, :] = cnt[i * highs : (i + 1) * highs, LANES:]
        return carry

    lax.fori_loop(0, groups * prow // 2 // unroll, step, 0)
    total = groups * nbags
    acc = jnp.zeros((total, table_ref.shape[1]), jnp.float32)
    for h in range(highs):
        at = pl.ds(h, total, stride=highs)
        counts = jnp.concatenate([cnt0_ref[at, :].astype(jnp.bfloat16), cnt1_ref[at, :].astype(jnp.bfloat16)], axis=1)
        acc += jnp.dot(counts, table_ref[h * LOW : (h + 1) * LOW, :], preferred_element_type=jnp.float32)
    out_ref[...] = acc.reshape(groups, nbags, table_ref.shape[1])


def pool(base, keys, table):
    groups, (length, nbags), (rows, width) = len(keys), keys[0].shape, table.shape
    highs, total = rows // LOW, groups * nbags
    vmem = pl.BlockSpec(memory_space=pltpu.VMEM)
    lanes = pltpu.VMEM((total * length // LANES, LANES), jnp.float32)
    counts = pltpu.VMEM((total * highs, LANES), jnp.float32)
    return pl.pallas_call(
        functools.partial(pool_kernel, groups=groups, highs=highs, length=length, unroll=8),
        out_shape=jax.ShapeDtypeStruct((groups, nbags, width), jnp.float32),
        in_specs=[pl.BlockSpec(memory_space=pltpu.SMEM)] + [vmem] * (groups + 1),
        out_specs=vmem,
        scratch_shapes=[lanes, lanes, counts, counts],
        cost_estimate=pl.CostEstimate(
            flops=4 * total * rows * width, bytes_accessed=rows * width * 2, transcendentals=0
        ),
        compiler_params=pltpu.CompilerParams(vmem_limit_bytes=40 << 20),
    )(base, *keys, table)


def swap(value, axis, size, bit):
    return lax.ppermute(value, axis, [(i, i ^ bit) for i in range(size)])


def on_device(rows_size, rep_size, item_table, history_ids, history_mask):
    rows_dev = item_table.shape[0]
    block = lax.axis_index("rep") * rows_size + lax.axis_index("rows")
    base = (block * rows_dev).astype(jnp.int32).reshape(1)
    key = jnp.where(history_mask > 0, history_ids, -1).T
    keys = [key] + [swap(key, "rows", rows_size, s) for s in range(1, rows_size)]
    near = pool(base, keys[:2], item_table)
    sums = [near[0], near[1]]
    mine = sums[0] + swap(sums[1], "rows", rows_size, 1)
    far = []
    for s in range(2, rows_size, 2):
        part = pool(base, keys[s : s + 2], item_table)
        far.append(part[0] + swap(part[1], "rows", rows_size, 1))
    sums = [mine] + far
    while len(sums) > 1:
        half = len(sums) // 2
        sums = [a + swap(b, "rows", rows_size, 2 * half) for a, b in zip(sums[:half], sums[half:])]
    pooled = sums[0]
    bit = 1
    while bit < rep_size:
        pooled = pooled + swap(pooled, "rep", rep_size, bit)
        bit *= 2
    return pooled / jnp.sqrt(jnp.mean(pooled * pooled, axis=1, keepdims=True) + 1e-06)


def solution(mesh):
    body = functools.partial(on_device, mesh.shape["rows"], mesh.shape["rep"])
    return jax.shard_map(
        body,
        mesh=mesh,
        in_specs=(P(("rep", "rows"), None), P("rows", None), P("rows", None)),
        out_specs=P("rows", None),
        check_vma=False,
    )
```

```python
import functools

import jax
import jax.numpy as jnp
from jax import lax
from jax.experimental import pallas as pl
from jax.experimental.pallas import tpu as pltpu
from jax.sharding import PartitionSpec as P

LANES = 128
GAP = 4


def pool_kernel(key_ref, own_hbm, other_ref, out_ref, own_ref, m_ref, low_ref, cnt_ref, sem, *, highs):
    load = pltpu.make_async_copy(own_hbm, own_ref, sem)
    load.start()
    length, nbags = key_ref.shape
    per = LANES // length
    prow = nbags // per
    lane = lax.broadcasted_iota(jnp.int32, (prow, LANES), 1)
    odd = lax.broadcasted_iota(jnp.int32, (prow, LANES), 0) & 1
    keys = jnp.concatenate([key_ref[...]] * per, axis=0).T
    local = keys[:prow]
    for j in range(1, per):
        local = jnp.where(lane >= j * length, keys[j * prow : (j + 1) * prow], local)
    m = lax.shift_right_arithmetic(local, LANES.bit_length() - 1) + highs * (lane // length + per * odd)
    m_ref[...] = jnp.where(local >= 0, m, -1).astype(jnp.float32)
    low_ref[...] = (local & (LANES - 1)).astype(jnp.float32)
    pitch = nbags + GAP
    nums = lax.broadcasted_iota(jnp.int32, (max(2 * per * highs, LANES), LANES), 0)
    nums = nums.astype(jnp.float32).astype(jnp.bfloat16)
    one, zero = jnp.bfloat16(1), jnp.bfloat16(0)

    def hot(row, n):
        row = jnp.broadcast_to(row, (16, LANES)).astype(jnp.bfloat16)
        return jnp.concatenate([jnp.where(nums[k : k + 16] == row, one, zero) for k in range(0, n, 16)], axis=0)

    for p in range(0, prow, 2):
        lhs = jnp.concatenate([hot(m_ref[k : k + 1, :], 2 * per * highs) for k in (p, p + 1)], axis=1)
        rhs = jnp.concatenate([hot(low_ref[k : k + 1, :], LANES) for k in (p, p + 1)], axis=1)
        cnt = lax.dot_general(lhs, rhs, (((1,), (1,)), ((), ())), preferred_element_type=jnp.float32)
        for i in range(2 * per):
            bag = (i % per) * prow + p + i // per
            for h in range(0, highs, 8):
                cnt_ref[pl.ds(h * pitch + bag, 8, stride=pitch), :] = cnt[i * highs + h : i * highs + h + 8, :]
    acc = jnp.zeros(out_ref.shape, jnp.float32)
    load.wait()
    for h in range(0, highs, 2):
        counts = [cnt_ref[k * pitch : k * pitch + nbags, :].astype(jnp.bfloat16) for k in (h, h + 1)]
        table, at = (own_ref, h) if 2 * h < highs else (other_ref, h - highs // 2)
        rows = table[at * LANES : (at + 2) * LANES, :]
        acc += jnp.dot(jnp.concatenate(counts, axis=1), rows, preferred_element_type=jnp.float32)
    out_ref[...] = acc


def pool(key, own, other):
    (length, nbags), (rows, width) = key.shape, own.shape
    highs = 2 * rows // LANES
    vmem = pl.BlockSpec(memory_space=pltpu.VMEM)
    packed = pltpu.VMEM((nbags * length // LANES, LANES), jnp.float32)
    return pl.pallas_call(
        functools.partial(pool_kernel, highs=highs),
        out_shape=jax.ShapeDtypeStruct((nbags, width), jnp.float32),
        in_specs=[vmem, pl.BlockSpec(memory_space=pltpu.HBM), vmem],
        out_specs=vmem,
        scratch_shapes=[
            pltpu.VMEM(own.shape, own.dtype),
            packed,
            packed,
            pltpu.VMEM((highs * (nbags + GAP), LANES), jnp.float32),
            pltpu.SemaphoreType.DMA,
        ],
        cost_estimate=pl.CostEstimate(
            flops=8 * nbags * rows * width, bytes_accessed=rows * width * 4, transcendentals=0
        ),
        compiler_params=pltpu.CompilerParams(vmem_limit_bytes=32 << 20),
    )(key, own, other)


def swap(value, axis, size, bit):
    return lax.ppermute(value, axis, [(i, i ^ bit) for i in range(size)])


def on_device(rows_size, rep_size, item_table, history_ids, history_mask):
    rows_dev = item_table.shape[0]
    other = swap(item_table, "rows", rows_size, 1)
    row, rep = lax.axis_index("rows"), lax.axis_index("rep")

    def key_for(s):
        there = row ^ s
        local = history_ids - (rep * rows_size + (there & -2)) * rows_dev
        used = (history_mask > 0) & (local >= 0) & (local < 2 * rows_dev)
        return jnp.where(used, local ^ ((there & 1) * rows_dev), -1).T

    keys = [swap(key_for(s), "rows", rows_size, s) for s in range(2, rows_size, 2)]
    near = pool(key_for(0), item_table, other)
    keys, near = lax.optimization_barrier((keys, near))
    sums = [near] + [pool(k, item_table, other) for k in keys]
    while len(sums) > 1:
        half = len(sums) // 2
        sums = [a + swap(b, "rows", rows_size, 2 * half) for a, b in zip(sums[:half], sums[half:])]
    pooled = sums[0]
    bit = 1
    while bit < rep_size:
        pooled = pooled + swap(pooled, "rep", rep_size, bit)
        bit *= 2
    return pooled / jnp.sqrt(jnp.mean(pooled * pooled, axis=1, keepdims=True) + 1e-06)


def solution(mesh):
    body = functools.partial(on_device, mesh.shape["rows"], mesh.shape["rep"])
    return jax.shard_map(
        body,
        mesh=mesh,
        in_specs=(P(("rep", "rows"), None), P("rows", None), P("rows", None)),
        out_specs=P("rows", None),
        check_vma=False,
    )
```

```python
import functools

import jax
import jax.numpy as jnp
from jax import lax
from jax.experimental import pallas as pl
from jax.experimental.pallas import tpu as pltpu
from jax.sharding import PartitionSpec as P

LANES = 128
GAP = 4


def count(key_ref, m_ref, low_ref, cnt_ref, highs):
    length, nbags = key_ref.shape
    per = LANES // length
    prow = nbags // per
    lane = lax.broadcasted_iota(jnp.int32, (prow, LANES), 1)
    odd = lax.broadcasted_iota(jnp.int32, (prow, LANES), 0) & 1
    keys = jnp.concatenate([key_ref[...]] * per, axis=0).T
    local = keys[:prow]
    for j in range(1, per):
        local = jnp.where(lane >= j * length, keys[j * prow : (j + 1) * prow], local)
    row = lax.axis_index("rows")
    half = highs // 2 * LANES
    local = local - (lax.axis_index("rep") * lax.axis_size("rows") + (row & -2)) * half
    inside = (local >= 0) & (local < 2 * half)
    local = local ^ ((row & 1) * half)
    m = lax.shift_right_arithmetic(local, LANES.bit_length() - 1) + highs * (lane // length + per * odd)
    m_ref[...] = jnp.where(inside, m, -1).astype(jnp.float32)
    low_ref[...] = (local & (LANES - 1)).astype(jnp.float32)
    pitch = nbags + GAP
    nums = lax.broadcasted_iota(jnp.int32, (max(2 * per * highs, LANES), LANES), 0)
    nums = nums.astype(jnp.float32).astype(jnp.bfloat16)
    one, zero = jnp.bfloat16(1), jnp.bfloat16(0)

    def hot(row, n):
        row = jnp.broadcast_to(row, (16, LANES)).astype(jnp.bfloat16)
        return jnp.concatenate([jnp.where(nums[k : k + 16] == row, one, zero) for k in range(0, n, 16)], axis=0)

    for p in range(0, prow, 2):
        lhs = jnp.concatenate([hot(m_ref[k : k + 1, :], 2 * per * highs) for k in (p, p + 1)], axis=1)
        rhs = jnp.concatenate([hot(low_ref[k : k + 1, :], LANES) for k in (p, p + 1)], axis=1)
        cnt = lax.dot_general(lhs, rhs, (((1,), (1,)), ((), ())), preferred_element_type=jnp.float32)
        for i in range(2 * per):
            bag = (i % per) * prow + p + i // per
            for h in range(0, highs, 8):
                cnt_ref[pl.ds(h * pitch + bag, 8, stride=pitch), :] = cnt[i * highs + h : i * highs + h + 8, :]


def product(cnt_ref, own_ref, other_ref, out_ref, highs):
    nbags = out_ref.shape[0]
    pitch = nbags + GAP
    acc = jnp.zeros(out_ref.shape, jnp.float32)
    for h in range(0, highs, 2):
        counts = [cnt_ref[k * pitch : k * pitch + nbags, :].astype(jnp.bfloat16) for k in (h, h + 1)]
        table, at = (own_ref, h) if 2 * h < highs else (other_ref, h - highs // 2)
        rows = table[at * LANES : (at + 2) * LANES, :]
        acc += jnp.dot(jnp.concatenate(counts, axis=1), rows, preferred_element_type=jnp.float32)
    out_ref[...] = acc


def count_kernel(key_ref, cnt_ref, m_ref, low_ref, *, highs):
    count(key_ref, m_ref, low_ref, cnt_ref, highs)


def product_kernel(cnt_ref, own_ref, other_ref, out_ref, *, highs):
    product(cnt_ref, own_ref, other_ref, out_ref, highs)


def pool_kernel(key_ref, own_ref, other_ref, out_ref, m_ref, low_ref, cnt_ref, *, highs):
    count(key_ref, m_ref, low_ref, cnt_ref, highs)
    product(cnt_ref, own_ref, other_ref, out_ref, highs)


def pool(key, own, other, split):
    (length, nbags), (rows, width) = key.shape, own.shape
    highs = 2 * rows // LANES
    packed = pltpu.VMEM((nbags * length // LANES, LANES), jnp.float32)
    counts = (highs * (nbags + GAP), LANES)

    def call(kernel, operands, out, scratch, flops):
        return pl.pallas_call(
            functools.partial(kernel, highs=highs),
            out_shape=jax.ShapeDtypeStruct(out, jnp.float32),
            in_specs=[pl.BlockSpec(memory_space=pltpu.VMEM)] * len(operands),
            out_specs=pl.BlockSpec(memory_space=pltpu.VMEM),
            scratch_shapes=scratch,
            cost_estimate=pl.CostEstimate(flops=flops, bytes_accessed=0, transcendentals=0),
            compiler_params=pltpu.CompilerParams(vmem_limit_bytes=16 << 20),
        )(*operands)

    flops = 4 * nbags * rows * width
    if split:
        cnt = call(count_kernel, (key,), counts, [packed, packed], 2 * flops)
        return call(product_kernel, (cnt, own, other), (nbags, width), [], flops)
    scratch = [packed, packed, pltpu.VMEM(counts, jnp.float32)]
    return call(pool_kernel, (key, own, other), (nbags, width), scratch, 3 * flops)


def swap(value, axis, size, bit):
    return lax.ppermute(value, axis, [(i, i ^ bit) for i in range(size)])


def on_device(rows_size, rep_size, item_table, history_ids, history_mask):
    other = swap(item_table, "rows", rows_size, 1)
    key = jnp.where(history_mask > 0, history_ids, -1).T
    keys = [swap(key, "rows", rows_size, s) for s in range(2, rows_size, 2)]
    near = pool(key, item_table, other, True)
    keys, near = lax.optimization_barrier((keys, near))
    def hop(value, row_bit, rep_bit):
        both = rep_bit * rows_size + row_bit
        return lax.ppermute(value, ("rep", "rows"), [(i, i ^ both) for i in range(rows_size * rep_size)])

    sums = [near] + [pool(k, item_table, other, False) for k in keys]
    while len(sums) > 2:
        half = len(sums) // 2
        sums = [a + swap(b, "rows", rows_size, 2 * half) for a, b in zip(sums[:half], sums[half:])]
    near, far = sums
    pooled = near + hop(near, 0, 1) + (hop(far, 2, 0) + hop(far, 2, 1))
    bit = 2
    while 2 * bit < rep_size:
        pooled = pooled + hop(pooled, 0, 1 * bit) + (hop(pooled, 0, 3 * bit) + hop(pooled, 0, 2 * bit))
        bit *= 4
    while bit < rep_size:
        pooled = pooled + hop(pooled, 0, bit)
        bit *= 2
    return pooled / jnp.sqrt(jnp.mean(pooled * pooled, axis=1, keepdims=True) + 1e-06)


def solution(mesh):
    body = functools.partial(on_device, mesh.shape["rows"], mesh.shape["rep"])
    return jax.shard_map(
        body,
        mesh=mesh,
        in_specs=(P(("rep", "rows"), None), P("rows", None), P("rows", None)),
        out_specs=P("rows", None),
        check_vma=False,
    )
```

```python
import functools

import jax
import jax.numpy as jnp
from jax import lax
from jax.experimental import pallas as pl
from jax.experimental.pallas import tpu as pltpu
from jax.sharding import PartitionSpec as P


LANES = 128
GAP = 4


def count(key_ref, m_ref, low_ref, cnt_ref, highs):
    length, nbags = key_ref.shape
    per = LANES // length
    prow = nbags // per
    lane = lax.broadcasted_iota(jnp.int32, (prow, LANES), 1)
    odd = lax.broadcasted_iota(jnp.int32, (prow, LANES), 0) & 1
    keys = jnp.concatenate([key_ref[...]] * per, axis=0).T
    local = keys[:prow]
    for j in range(1, per):
        local = jnp.where(lane >= j * length, keys[j * prow : (j + 1) * prow], local)
    row = lax.axis_index("rows")
    half = highs // 2 * LANES
    local = local - (lax.axis_index("rep") * lax.axis_size("rows") + (row & -2)) * half
    inside = (local >= 0) & (local < 2 * half)
    local = local ^ ((row & 1) * half)
    m = lax.shift_right_arithmetic(local, LANES.bit_length() - 1) + highs * (lane // length + per * odd)
    m_ref[...] = jnp.where(inside, m, -1).astype(jnp.float32)
    low_ref[...] = (local & (LANES - 1)).astype(jnp.float32)
    pitch = nbags + GAP
    nums = lax.broadcasted_iota(jnp.int32, (max(2 * per * highs, LANES), LANES), 0)
    nums = nums.astype(jnp.float32).astype(jnp.bfloat16)
    one, zero = jnp.bfloat16(1), jnp.bfloat16(0)

    def hot(row, n):
        row = jnp.broadcast_to(row, (16, LANES)).astype(jnp.bfloat16)
        tiles = [jnp.where(nums[k : k + 16] == row, one, zero) for k in range(0, n, 16)]
        return jnp.concatenate(tiles, axis=0).astype(jnp.float8_e4m3fn)

    for p in range(0, prow, 2):
        lhs = jnp.concatenate([hot(m_ref[k : k + 1, :], 2 * per * highs) for k in (p, p + 1)], axis=1)
        rhs = jnp.concatenate([hot(low_ref[k : k + 1, :], LANES) for k in (p, p + 1)], axis=1)
        cnt = lax.dot_general(lhs, rhs, (((1,), (1,)), ((), ())), preferred_element_type=jnp.float32)
        for i in range(2 * per):
            bag = (i % per) * prow + p + i // per
            for h in range(0, highs, 8):
                cnt_ref[pl.ds(h * pitch + bag, 8, stride=pitch), :] = cnt[i * highs + h : i * highs + h + 8, :]


def product(cnt_ref, own_ref, other_ref, out_ref, highs):
    nbags = out_ref.shape[0]
    pitch = nbags + GAP
    acc = jnp.zeros(out_ref.shape, jnp.float32)
    for h in range(0, highs, 2):
        counts = [cnt_ref[k * pitch : k * pitch + nbags, :].astype(jnp.bfloat16) for k in (h, h + 1)]
        table, at = (own_ref, h) if 2 * h < highs else (other_ref, h - highs // 2)
        rows = table[at * LANES : (at + 2) * LANES, :]
        acc += jnp.dot(jnp.concatenate(counts, axis=1), rows, preferred_element_type=jnp.float32)
    out_ref[...] = acc


def count_kernel(key_ref, cnt_ref, m_ref, low_ref, *, highs):
    count(key_ref, m_ref, low_ref, cnt_ref, highs)


def product_kernel(cnt_ref, own_ref, other_ref, out_ref, *, highs):
    product(cnt_ref, own_ref, other_ref, out_ref, highs)


def pool_kernel(key_ref, own_ref, other_ref, out_ref, m_ref, low_ref, cnt_ref, *, highs):
    count(key_ref, m_ref, low_ref, cnt_ref, highs)
    product(cnt_ref, own_ref, other_ref, out_ref, highs)


def pool(key, own, other, split):
    (length, nbags), (rows, width) = key.shape, own.shape
    highs = 2 * rows // LANES
    packed = pltpu.VMEM((nbags * length // LANES, LANES), jnp.float32)
    counts = (highs * (nbags + GAP), LANES)

    def call(kernel, operands, out, scratch, flops):
        return pl.pallas_call(
            functools.partial(kernel, highs=highs),
            out_shape=jax.ShapeDtypeStruct(out, jnp.float32),
            in_specs=[pl.BlockSpec(memory_space=pltpu.VMEM)] * len(operands),
            out_specs=pl.BlockSpec(memory_space=pltpu.VMEM),
            scratch_shapes=scratch,
            cost_estimate=pl.CostEstimate(flops=flops, bytes_accessed=0, transcendentals=0),
            compiler_params=pltpu.CompilerParams(vmem_limit_bytes=16 << 20),
        )(*operands)

    flops = 4 * nbags * rows * width
    if split:
        cnt = call(count_kernel, (key,), counts, [packed, packed], 2 * flops)
        return call(product_kernel, (cnt, own, other), (nbags, width), [], flops)
    scratch = [packed, packed, pltpu.VMEM(counts, jnp.float32)]
    return call(pool_kernel, (key, own, other), (nbags, width), scratch, 3 * flops)


def swap(value, axis, size, bit):
    return lax.ppermute(value, axis, [(i, i ^ bit) for i in range(size)])


def on_device(rows_size, rep_size, item_table, history_ids, history_mask):
    other = swap(item_table, "rows", rows_size, 1)
    key = jnp.where(history_mask > 0, history_ids, -1).T

    def hop(value, row_bit, rep_bit):
        both = rep_bit * rows_size + row_bit
        return lax.ppermute(value, ("rep", "rows"), [(i, i ^ both) for i in range(rows_size * rep_size)])

    keys = []
    for s in range(2, rows_size, 2):
        keys.append(swap(key, "rows", rows_size, s))
    near = pool(key, item_table, other, True)
    sums = []
    for s, k in zip(range(2, rows_size, 2), keys):
        sums.append(pool(k, item_table, other, False))
    sums = [near] + sums
    while len(sums) > 2:
        half = len(sums) // 2
        sums = [a + swap(b, "rows", rows_size, 2 * half) for a, b in zip(sums[:half], sums[half:])]
    near, far = sums
    across = hop(near, 0, 1)
    straight = hop(far, 2, 0)
    crossed = hop(far, 2, 1)
    pooled = near + across + (straight + crossed)
    bit = 2
    while bit < rep_size:
        parts = []
        for k in (1, 2, 3) if 2 * bit < rep_size else (1,):
            parts.append(hop(pooled, 0, k * bit))
        pooled = pooled + sum(parts[1:], parts[0])
        bit *= 4
    return pooled / jnp.sqrt(jnp.mean(pooled * pooled, axis=1, keepdims=True) + 1e-06)


def solution(mesh):
    body = functools.partial(on_device, mesh.shape["rows"], mesh.shape["rep"])
    return jax.shard_map(
        body,
        mesh=mesh,
        in_specs=(P(("rep", "rows"), None), P("rows", None), P("rows", None)),
        out_specs=P("rows", None),
        check_vma=False,
    )
```
